256 devices in a mesh: slab: 64 (over z, x, core), rep: 4 (over y).
Axes of the slice: x: 4, y: 4, z: 8, core: 2. Of those that a mesh axis runs over, the one named last changes fastest.
Arguments:
- dipoles: float32 [24, 4096, 256], P('rep', 'slab'), parts along dimension 0, may hold values from -6 to 6
- inv_alpha: float32 [4096, 256], P('slab'), may hold values from 0.5 to 2
- row_site: int32 [2, 4096], P(None, 'slab'), may hold values from -1 to 63, as said below
- green: float32 [6, 128, 128, 512], P(None, None, 'slab'), may hold values from -6 to 6
Outputs:
- applied: float32 [24, 4096, 256], P('rep', 'slab'), parts along dimension 0
The draws below stay inside these ranges and needn't reach their ends.
There are 4 independent parts, one for each index of `rep`. The reference program is written for one: setup_inputs(seed, part) draws one part's arguments, and reference() takes and returns one part's arrays. A program takes and returns all parts, laid end to end along the dimension named above; an argument that names none is the same for every part. Nothing has to cross between parts.
Inputs may be any that keep to these rules, and one draw needn't show every extreme that they name: `row_site`: slot r belongs to device r // 64 of slab. A live slot has y under 128 / 2 and z under 128 / 2; an empty slot has -1 in both entries. Live slots name distinct (y, z). Of one device's slots, at most 2 have z in any one block of 2 consecutive planes, and in every draw some block gets exactly 2 from every device.
All inputs are finite; a program needn't handle non-finite values.
Results may differ from the reference program's by a relative error of at most 0.00005.
Values sent between devices are 32-bit elements; how exact they have to be, the bound alone decides.
No kernel may reach another device: no remote copies, remote signals or barrier semaphores. Data moves between devices by JAX's collectives and lax.ppermute only.
A program may use at most 64 MiB of HBM per device.

```python
import jax
import jax.numpy as jnp

NX = 256
NY = 128
NZ = 128
CAP = 2
LX = 128
ROWS = 4096
N_SLAB = 64


def draw_row_site(key, part):
    devices = N_SLAB
    planes = NZ // N_SLAB
    owners = N_SLAB // 2
    candidates = NY // 2 * planes
    key_count, key_level, key_full, key_order, key_slots = jax.random.split(jax.random.fold_in(key, 11), 5)
    counts = jax.random.randint(key_count, (devices, owners), 0, CAP + 1)
    levels = jax.random.randint(key_level, (devices, 1), 2, 9)
    counts = jnp.minimum(CAP, counts * levels // 4)
    full_owner = jax.random.randint(key_full, (), 0, owners)
    counts = jnp.where(jnp.arange(owners)[None, :] == full_owner, CAP, counts)
    scores = jax.random.randint(key_order, (owners, candidates), 0, 2 ** 20) * candidates + jnp.arange(candidates)[None, :]
    ordering = jnp.argsort(scores, axis=1)
    picked = ordering[:, :devices * CAP].reshape(owners, devices, CAP).transpose(1, 0, 2)
    occupied = jnp.arange(CAP)[None, None, :] < counts[:, :, None]
    cell_y = jnp.where(occupied, picked // planes, -1).reshape(devices, owners * CAP)
    cell_z = jnp.where(occupied, jnp.arange(owners)[None, :, None] * planes + picked % planes, -1).reshape(devices, owners * CAP)
    slot_scores = jax.random.randint(key_slots, (devices, owners * CAP), 0, 2 ** 20) * (owners * CAP) + jnp.arange(owners * CAP)[None, :]
    shuffle = jnp.argsort(slot_scores, axis=1)
    cell_y = jnp.take_along_axis(cell_y, shuffle, axis=1)
    cell_z = jnp.take_along_axis(cell_z, shuffle, axis=1)
    return jnp.stack([cell_y.reshape(-1), cell_z.reshape(-1)]).astype(jnp.int32)


def shard_levels(rng, extent, cuts, smallest, largest):
    factor_of = 1.0
    for axis_at, parts in cuts:
        heights = jax.random.uniform(jax.random.fold_in(jax.random.fold_in(rng, 6), axis_at), (parts,), jnp.float32, smallest / len(cuts), largest / len(cuts))
        factor_of = factor_of * jnp.repeat(jnp.exp(heights), extent[axis_at] // parts).reshape((-1,) + (1,) * (len(extent) - 1 - axis_at))
    return factor_of


def centred(rng, extent, scale, reach, shards=(), held_as=jnp.bfloat16):
    level = shard_levels(rng, extent, shards, -0.22, 0.18) if shards else 1.0
    values = jax.random.normal(rng, extent, jnp.float32) * scale * level
    return jnp.minimum(jnp.maximum(values, -reach), reach).astype(held_as)


def setup_inputs(seed: int = 0, part: int = 0) -> dict:
    keys = jax.random.split(jax.random.key(seed), 5)
    part_splits = jax.random.split(jax.random.fold_in(keys[4], part), 5)
    dipoles = centred(part_splits[0], (6, ROWS, 2 * LX), 1.0, 6.0, ((1, 64),), jnp.float32)
    inv_alpha = jnp.clip(0.5 + 1.5 * jax.random.uniform(keys[1], (ROWS, 2 * LX), jnp.float32) ** shard_levels(keys[1], (ROWS, 2 * LX), ((0, 64),), -0.2, 0.2), 0.5, 2.0)
    row_site = draw_row_site(jax.random.fold_in(keys[4], 71), part)
    green = centred(keys[3], (6, NZ, NY, 2 * NX), 1.0, 6.0, ((2, 64),), jnp.float32)
    return dict(dipoles=dipoles, inv_alpha=inv_alpha, row_site=row_site, green=green)


def reference(dipoles, inv_alpha, row_site, green):
    occupied = row_site[0] >= 0
    cell_y = jnp.where(occupied, row_site[0], 0).astype(jnp.int32)
    cell_z = jnp.where(occupied, row_site[1], 0).astype(jnp.int32)
    row_mask = occupied.astype(jnp.float32)[None, :, None]
    source = dipoles * row_mask
    grid_values = jnp.zeros((6, NZ, NY, 2 * LX), jnp.float32).at[:, cell_z, cell_y, :].add(source)
    field = grid_values[..., :LX] + 1j * grid_values[..., LX:]
    field = jnp.pad(field, ((0, 0), (0, 0), (0, 0), (0, NX - LX)))
    spectrum = jnp.fft.fftn(field, axes=(1, 2, 3)).reshape(2, 3, NZ, NY, NX)
    kernel = green[..., :NX] + 1j * green[..., NX:]
    sym_index = ((0, 1, 2), (1, 3, 4), (2, 4, 5))
    image = jnp.stack([sum(kernel[sym_index[target][other]] * spectrum[:, other] for other in range(3)) for target in range(3)], axis=1)
    potential = jnp.fft.ifftn(image, axes=(2, 3, 4)).reshape(6, NZ, NY, NX)[..., :LX]
    picked = potential[:, cell_z, cell_y, :]
    conv_re = picked.real.astype(jnp.float32)
    conv_im = picked.imag.astype(jnp.float32)
    alpha_re = inv_alpha[:, :LX]
    alpha_im = inv_alpha[:, LX:]
    dip_re = dipoles[:, :, :LX]
    dip_im = dipoles[:, :, LX:]
    out_re = alpha_re * dip_re - alpha_im * dip_im - conv_re
    out_im = alpha_re * dip_im + alpha_im * dip_re - conv_im
    return jnp.concatenate([out_re, out_im], axis=-1) * row_mask
```

```python
import math

import jax
import jax.numpy as jnp
import numpy as np
from jax import lax
from jax.experimental import pallas as pl
from jax.experimental.pallas import tpu as pltpu
from jax.sharding import PartitionSpec as P

NX = 256
NY = 128
NZ = 128
LX = 128
DEVICES = 64
BLOCKS = 32
INTERPRET = False

F32 = jnp.float32
BF16 = jnp.bfloat16


def split_table(table):
    high = np.asarray(table, np.float32).astype(BF16)
    low = (table - high.astype(np.float64)).astype(np.float32).astype(BF16)
    return high, low


def phases(rows, columns, length, sign):
    angles = 2.0 * math.pi * (np.outer(rows, columns) % length) / length
    return np.cos(angles), sign * np.sin(angles)


def tables():
    y = np.arange(NY // 2)
    ky = np.arange(NY)
    z = np.concatenate([np.arange(0, NZ // 2, 2), np.arange(1, NZ // 2, 2)])
    kz = np.arange(NZ)
    x = np.arange(LX)
    kx = np.arange(NX)
    cos, sin = phases(ky, y, NY, -1.0)
    y_high, y_low = split_table(np.concatenate([cos, sin]))
    y_forward = np.concatenate([y_high, y_low])
    cos, sin = phases(y, ky, NY, 1.0)
    y_high, y_low = split_table(np.concatenate([cos, sin], axis=1) / NY)
    y_back = np.concatenate([y_high, y_low], axis=1)
    cos, sin = phases(x, kx, NX, -1.0)
    x_forward = split_table(np.block([[cos, sin], [-sin, cos]]))
    cos, sin = phases(kx, x, NX, 1.0)
    x_back = split_table(np.block([[cos, sin], [-sin, cos]]) / NX)
    cos, sin = phases(kz, z, NZ, -1.0)
    z_forward = split_table(np.block([[cos, -sin], [sin, cos]]))
    cos, sin = phases(z, kz, NZ, 1.0)
    z_back = split_table(np.block([[cos, -sin], [sin, cos]]) / NZ)
    return y_forward, y_back, x_forward, x_back, z_forward, z_back


def halves(values):
    high = values.astype(BF16)
    return high, (values - high.astype(F32)).astype(BF16)


def thirds(values):
    high = values.astype(BF16)
    rest = values - high.astype(F32)
    middle = rest.astype(BF16)
    return high, middle, (rest - middle.astype(F32)).astype(BF16)


def dot(left, right):
    return jnp.dot(left, right, preferred_element_type=F32)


def dot_split(left, right):
    return dot(left[0], right[0]) + (dot(left[0], right[1]) + dot(left[1], right[0]))


def pick_rows(hot, values):
    high, middle, low = thirds(values)
    return dot(hot, high) + dot(hot, middle) + dot(hot, low)


def grid_index(shape, axis):
    return lax.broadcasted_iota(jnp.int32, shape, axis)


def to_column(row):
    n = row.shape[1]
    diagonal = grid_index((n, n), 0) == grid_index((n, n), 1)
    return jnp.sum(jnp.where(diagonal, row, 0), axis=1, keepdims=True)


def row_targets(site_ref):
    cell_y = site_ref[0:1, :]
    cell_z = site_ref[1:2, :]
    block = jnp.where(cell_y >= 0, cell_z // 2, -1)
    n = block.shape[1]
    earlier = grid_index((n, n), 0) < grid_index((n, n), 1)
    same = (to_column(block) == block) & earlier
    rank = jnp.sum(same.astype(jnp.int32), axis=0, keepdims=True)
    target = jnp.where(cell_y >= 0, rank * BLOCKS + block, -1)
    return target, (cell_z % 2) * (NY // 2) + cell_y


def pack_kernel(site_ref, dipoles_ref, out_ref):
    target, place = row_targets(site_ref)
    n = target.shape[1]
    chosen = grid_index((n, n), 0) == target
    hot = chosen.astype(BF16)
    for c in range(6):
        v, j = divmod(c, 3)
        rows = pick_rows(hot, dipoles_ref[c])
        for t in range(2):
            for p in range(2):
                out_ref[pl.ds(13 * v + 6 * t + 2 * j + p, BLOCKS, stride=26), :] = rows[
                    t * BLOCKS : (t + 1) * BLOCKS, p * LX : (p + 1) * LX
                ]
    places = jnp.sum(jnp.where(chosen, place + 1, 0), axis=1, keepdims=True) - 1
    places = places.astype(F32)
    lanes = grid_index((BLOCKS, LX), 1)
    row = jnp.where(lanes == 0, places[:BLOCKS], places[BLOCKS:])
    for v in range(2):
        out_ref[pl.ds(13 * v + 12, BLOCKS, stride=26), :] = row


def slot_places(received_ref):
    rows = received_ref[pl.ds(12, DEVICES, stride=13), :]
    return jnp.concatenate([rows[:, 0:1], rows[:, 1:2]], axis=0).astype(jnp.int32)


def y_forward_kernel(received_ref, table_ref, out_ref):
    slots = 2 * DEVICES
    column = slot_places(received_ref)
    diagonal = grid_index((slots, slots), 0) == grid_index((slots, slots), 1)
    row = jnp.sum(jnp.where(diagonal, column, 0), axis=0, keepdims=True)
    y = grid_index((NY // 2, slots), 0)
    hot = jnp.concatenate([(y == row).astype(BF16), (y + NY // 2 == row).astype(BF16)], axis=1)
    table = dot(table_ref[...], hot).astype(BF16)
    lefts = []
    for part in range(2):
        cos = table[part * 256 : part * 256 + 128]
        sin = table[part * 256 + 128 : part * 256 + 256]
        rows = []
        for zp in range(2):
            c = cos[:, zp * slots : (zp + 1) * slots]
            s = sin[:, zp * slots : (zp + 1) * slots]
            rows.append(jnp.concatenate([c, -s], axis=1))
            rows.append(jnp.concatenate([s, c], axis=1))
        lefts.append(jnp.concatenate(rows, axis=0))
    rights = []
    for j in range(3):
        pieces = []
        for p in range(2):
            for t in range(2):
                pieces.append(received_ref[pl.ds(6 * t + 2 * j + p, DEVICES, stride=13), :])
        rights.append(jnp.concatenate(pieces, axis=0))
    right = halves(jnp.concatenate(rights, axis=1))
    result = dot_split(lefts, right)
    for zp in range(2):
        for p in range(2):
            for j in range(3):
                out_ref[pl.ds(6 * zp + 2 * j + p, NY, stride=12), :] = result[
                    zp * 256 + p * 128 : zp * 256 + p * 128 + 128, j * 128 : (j + 1) * 128
                ]


SYMMETRIC = ((0, 1, 2), (1, 3, 4), (2, 4, 5))


def middle_kernel(
    received_ref,
    green_ref,
    xf_high,
    xf_low,
    xb_high,
    xb_low,
    zf_high,
    zf_low,
    zb_high,
    zb_low,
    out_ref,
):
    for g in range(4):
        ky = g % 2
        base = 12 * g
        rows = []
        for j in range(3):
            lanes = []
            for p in range(2):
                lanes.append(
                    jnp.concatenate(
                        [
                            received_ref[pl.ds(base + 6 * zp + 2 * j + p, BLOCKS, stride=48), :]
                            for zp in range(2)
                        ],
                        axis=0,
                    )
                )
            rows.append(jnp.concatenate(lanes, axis=1))
        lines = halves(jnp.concatenate(rows, axis=0))
        lines = dot_split(lines, (xf_high[...], xf_low[...]))
        planes = jnp.concatenate(
            [
                jnp.concatenate([lines[64 * j : 64 * j + 64, :NX], lines[64 * j : 64 * j + 64, NX:]], axis=0)
                for j in range(3)
            ],
            axis=1,
        )
        planes = dot_split((zf_high[...], zf_low[...]), halves(planes))
        images_re = []
        images_im = []
        for a in range(3):
            total_re = None
            for b in range(3):
                m = SYMMETRIC[a][b]
                kernel_re = green_ref[ky, m, :, :NX]
                kernel_im = green_ref[ky, m, :, NX:]
                source_re = planes[:NZ, b * NX : (b + 1) * NX]
                source_im = planes[NZ:, b * NX : (b + 1) * NX]
                term_re = kernel_re * source_re - kernel_im * source_im
                term_im = kernel_re * source_im + kernel_im * source_re
                total_re = term_re if b == 0 else total_re + term_re
                total_im = term_im if b == 0 else total_im + term_im
            images_re.append(total_re)
            images_im.append(total_im)
        images = jnp.concatenate(
            [jnp.concatenate(images_re, axis=1), jnp.concatenate(images_im, axis=1)], axis=0
        )
        planes = dot_split((zb_high[...], zb_low[...]), halves(images))
        lines = jnp.concatenate(
            [
                jnp.concatenate(
                    [planes[:64, j * NX : (j + 1) * NX], planes[64:, j * NX : (j + 1) * NX]], axis=1
                )
                for j in range(3)
            ],
            axis=0,
        )
        lines = dot_split(halves(lines), (xb_high[...], xb_low[...]))
        for j in range(3):
            for p in range(2):
                for zp in range(2):
                    first = 64 * j + BLOCKS * zp
                    out_ref[pl.ds(base + 6 * zp + 2 * j + p, BLOCKS, stride=48), :] = lines[
                        first : first + BLOCKS, p * LX : (p + 1) * LX
                    ]


def y_back_kernel(received_ref, first_ref, table_ref, out_ref):
    slots = 2 * DEVICES
    column = slot_places(first_ref)
    y = grid_index((slots, NY // 2), 1)
    hot = jnp.concatenate([(y == column).astype(BF16), (y + NY // 2 == column).astype(BF16)], axis=0)
    table = dot(hot, table_ref[...]).astype(BF16)
    lefts = []
    for part in range(2):
        cos = table[:, part * 256 : part * 256 + 128]
        sin = table[:, part * 256 + 128 : part * 256 + 256]
        c0, c1, s0, s1 = cos[:slots], cos[slots:], sin[:slots], sin[slots:]
        lefts.append(
            jnp.concatenate(
                [
                    jnp.concatenate([c0, c1, -s0, -s1], axis=1),
                    jnp.concatenate([s0, s1, c0, c1], axis=1),
                ],
                axis=0,
            )
        )
    rights = []
    for j in range(3):
        pieces = []
        for p in range(2):
            for zp in range(2):
                pieces.append(received_ref[pl.ds(6 * zp + 2 * j + p, NY, stride=12), :])
        rights.append(jnp.concatenate(pieces, axis=0))
    right = halves(jnp.concatenate(rights, axis=1))
    result = dot_split(lefts, right)
    for p in range(2):
        for t in range(2):
            for j in range(3):
                first = p * slots + t * DEVICES
                out_ref[pl.ds(6 * t + 2 * j + p, DEVICES, stride=12), :] = result[
                    first : first + DEVICES, j * 128 : (j + 1) * 128
                ]


def finish_kernel(received_ref, site_ref, dipoles_ref, alpha_ref, out_ref):
    target, _ = row_targets(site_ref)
    n = target.shape[1]
    target = to_column(target)
    hot = (grid_index((n, n), 1) == target).astype(BF16)
    live = target >= 0
    alpha_re = alpha_ref[:, :LX]
    alpha_im = alpha_ref[:, LX:]
    for c in range(6):
        v, j = divmod(c, 3)
        lanes = []
        for p in range(2):
            lanes.append(
                jnp.concatenate(
                    [
                        received_ref[pl.ds(12 * v + 6 * t + 2 * j + p, BLOCKS, stride=24), :]
                        for t in range(2)
                    ],
                    axis=0,
                )
            )
        rows = pick_rows(hot, jnp.concatenate(lanes, axis=1))
        dip_re = dipoles_ref[c, :, :LX]
        dip_im = dipoles_ref[c, :, LX:]
        out_ref[c, :, :LX] = jnp.where(live, alpha_re * dip_re - alpha_im * dip_im - rows[:, :LX], 0.0)
        out_ref[c, :, LX:] = jnp.where(live, alpha_re * dip_im + alpha_im * dip_re - rows[:, LX:], 0.0)


def call(kernel, shape, *operands, flops=0):
    whole = pl.BlockSpec(memory_space=pltpu.VMEM)
    return pl.pallas_call(
        kernel,
        out_shape=jax.ShapeDtypeStruct(shape, F32),
        in_specs=[whole] * len(operands),
        out_specs=whole,
        compiler_params=pltpu.CompilerParams(vmem_limit_bytes=48 * 1024 * 1024),
        cost_estimate=pl.CostEstimate(flops=flops, bytes_accessed=0, transcendentals=0),
        interpret=INTERPRET,
    )(*operands)


def exchange(rows):
    packed = rows.reshape(DEVICES, 1, rows.shape[0] // DEVICES * rows.shape[1])
    moved = lax.all_to_all(packed, "slab", split_axis=0, concat_axis=0, tiled=True)
    return moved.reshape(rows.shape)


def body(dipoles, inv_alpha, row_site, green):
    y_forward, y_back, x_forward, x_back, z_forward, z_back = tables()
    packed = call(pack_kernel, (13 * DEVICES, LX), row_site, dipoles)
    first = exchange(packed)
    planes = call(y_forward_kernel, (24 * DEVICES, LX), first, y_forward)
    pencils = exchange(planes)
    green_rows = jnp.transpose(green, (2, 0, 1, 3))
    images = call(
        middle_kernel,
        (24 * DEVICES, LX),
        pencils,
        green_rows,
        *x_forward,
        *x_back,
        *z_forward,
        *z_back,
    )
    planes = exchange(images)
    rows = call(y_back_kernel, (12 * DEVICES, LX), planes, first, y_back)
    returned = exchange(rows)
    return call(finish_kernel, dipoles.shape, returned, row_site, dipoles, inv_alpha)


def solution(mesh):
    return jax.shard_map(
        body,
        mesh=mesh,
        in_specs=(
            P("rep", "slab", None),
            P("slab", None),
            P(None, "slab"),
            P(None, None, "slab", None),
        ),
        out_specs=P("rep", "slab", None),
        check_vma=False,
    )
```

```python
import math

import jax
import jax.numpy as jnp
import numpy as np
from jax import lax
from jax.experimental import pallas as pl
from jax.experimental.pallas import tpu as pltpu
from jax.sharding import PartitionSpec as P

NX = 256
NY = 128
NZ = 128
LX = 128
DEVICES = 64
BLOCKS = 32
INTERPRET = False

F32 = jnp.float32
BF16 = jnp.bfloat16


def split_table(table):
    high = np.asarray(table, np.float32).astype(BF16)
    low = (table - high.astype(np.float64)).astype(np.float32).astype(BF16)
    return high, low


def phases(rows, columns, length, sign):
    angles = 2.0 * math.pi * (np.outer(rows, columns) % length) / length
    return np.cos(angles), sign * np.sin(angles)


def tables():
    y = np.arange(NY // 2)
    ky = np.arange(NY)
    z = np.concatenate([np.arange(0, NZ // 2, 2), np.arange(1, NZ // 2, 2)])
    kz = np.arange(NZ)
    x = np.arange(LX)
    kx = np.arange(NX)
    cos, sin = phases(ky, y, NY, -1.0)
    y_high, y_low = split_table(np.concatenate([cos, sin]))
    y_forward = np.concatenate([y_high, y_low])
    cos, sin = phases(y, ky, NY, 1.0)
    y_high, y_low = split_table(np.concatenate([cos, sin], axis=1) / NY)
    y_back = np.concatenate([y_high, y_low], axis=1)
    cos, sin = phases(x, kx, NX, -1.0)
    x_forward = split_table(np.block([[cos, sin], [-sin, cos]]))
    cos, sin = phases(kx, x, NX, 1.0)
    x_back = split_table(np.block([[cos, sin], [-sin, cos]]) / NX)
    cos, sin = phases(kz, z, NZ, -1.0)
    z_forward = split_table(np.block([[cos, -sin], [sin, cos]]))
    cos, sin = phases(z, kz, NZ, 1.0)
    z_back = split_table(np.block([[cos, -sin], [sin, cos]]) / NZ)
    y_rows = np.zeros((384, 256), BF16)
    y_rows[:256, :64] = y_forward[:256]
    y_rows[:256, 64:128] = y_forward[256:]
    y_rows[256:320] = y_back[:, :256]
    y_rows[320:384] = y_back[:, 256:]
    pieces = []
    for part in x_forward:
        pieces += [part[:, :NX], part[:, NX:]]
    for part in x_back:
        pieces += [part[:NX], part[NX:]]
    pieces.append(np.concatenate(z_forward, axis=1))
    pieces.append(np.concatenate(z_back, axis=0))
    return y_rows, np.stack(pieces)


def halves(values):
    high = values.astype(BF16)
    return high, (values - high.astype(F32)).astype(BF16)


def thirds(values):
    high = values.astype(BF16)
    rest = values - high.astype(F32)
    middle = rest.astype(BF16)
    return high, middle, (rest - middle.astype(F32)).astype(BF16)


def dot(left, right):
    return jnp.dot(left, right, preferred_element_type=F32)


def dot_split(left, right):
    return dot(left[0], right[0]) + (dot(left[0], right[1]) + dot(left[1], right[0]))


def pick_rows(hot, values):
    high, middle, low = thirds(values)
    return dot(hot, high) + dot(hot, middle) + dot(hot, low)


def grid_index(shape, axis):
    return lax.broadcasted_iota(jnp.int32, shape, axis)


def to_column(row):
    n = row.shape[1]
    diagonal = grid_index((n, n), 0) == grid_index((n, n), 1)
    return jnp.sum(jnp.where(diagonal, row, 0), axis=1, keepdims=True)


def row_targets(site_ref):
    cell_y = site_ref[0:1, :]
    cell_z = site_ref[1:2, :]
    block = jnp.where(cell_y >= 0, cell_z // 2, -1)
    n = block.shape[1]
    earlier = grid_index((n, n), 0) < grid_index((n, n), 1)
    same = (to_column(block) == block) & earlier
    rank = jnp.sum(same.astype(jnp.int32), axis=0, keepdims=True)
    target = jnp.where(cell_y >= 0, rank * BLOCKS + block, -1)
    return target, (cell_z % 2) * (NY // 2) + cell_y


def pack_kernel(site_ref, dipoles_ref, out_ref):
    target, place = row_targets(site_ref)
    n = target.shape[1]
    chosen = grid_index((n, n), 0) == target
    hot = chosen.astype(BF16)
    for c in range(6):
        v, j = divmod(c, 3)
        rows = pick_rows(hot, dipoles_ref[c])
        for t in range(2):
            for p in range(2):
                out_ref[pl.ds(13 * v + 6 * t + 2 * j + p, BLOCKS, stride=26), :] = rows[
                    t * BLOCKS : (t + 1) * BLOCKS, p * LX : (p + 1) * LX
                ]
    places = jnp.sum(jnp.where(chosen, place + 1, 0), axis=1, keepdims=True) - 1
    places = places.astype(F32)
    lanes = grid_index((BLOCKS, LX), 1)
    row = jnp.where(lanes == 0, places[:BLOCKS], places[BLOCKS:])
    for v in range(2):
        out_ref[pl.ds(13 * v + 12, BLOCKS, stride=26), :] = row


def slot_places(rows):
    return jnp.concatenate([rows[:, 0:1], rows[:, 1:2]], axis=0).astype(jnp.int32)


def y_forward_kernel(received_ref, table_ref, out_ref, places_ref):
    slots = 2 * DEVICES
    places = received_ref[pl.ds(12, DEVICES, stride=13), :]
    places_ref[...] = places
    column = slot_places(places)
    diagonal = grid_index((slots, slots), 0) == grid_index((slots, slots), 1)
    row = jnp.sum(jnp.where(diagonal, column, 0), axis=0, keepdims=True)
    y = grid_index((NY // 2, slots), 0)
    hot = jnp.concatenate([(y == row).astype(BF16), (y + NY // 2 == row).astype(BF16)], axis=1)
    none = jnp.zeros_like(hot)
    lefts = []
    for part in range(2):
        chooser = jnp.concatenate([none, hot] if part else [hot, none], axis=0)
        table = dot(table_ref[:256, :128], chooser).astype(BF16)
        cos = table[:128]
        sin = table[128:]
        rows = []
        for zp in range(2):
            c = cos[:, zp * slots : (zp + 1) * slots]
            s = sin[:, zp * slots : (zp + 1) * slots]
            rows.append(jnp.concatenate([c, -s], axis=1))
            rows.append(jnp.concatenate([s, c], axis=1))
        lefts.append(jnp.concatenate(rows, axis=0))
    rights = []
    for j in range(3):
        pieces = []
        for p in range(2):
            for t in range(2):
                pieces.append(received_ref[pl.ds(6 * t + 2 * j + p, DEVICES, stride=13), :])
        rights.append(jnp.concatenate(pieces, axis=0))
    right = halves(jnp.concatenate(rights, axis=1))
    result = dot_split(lefts, right)
    for zp in range(2):
        for p in range(2):
            for j in range(3):
                out_ref[pl.ds(6 * zp + 2 * j + p, NY, stride=12), :] = result[
                    zp * 256 + p * 128 : zp * 256 + p * 128 + 128, j * 128 : (j + 1) * 128
                ]


SYMMETRIC = ((0, 1, 2), (1, 3, 4), (2, 4, 5))


def middle_kernel(received_ref, green_ref, table_ref, out_ref):
    for g in range(4):
        ky = g % 2
        base = 12 * g
        rows = []
        for j in range(3):
            lanes = []
            for p in range(2):
                lanes.append(
                    jnp.concatenate(
                        [
                            received_ref[pl.ds(base + 6 * zp + 2 * j + p, BLOCKS, stride=48), :]
                            for zp in range(2)
                        ],
                        axis=0,
                    )
                )
            rows.append(jnp.concatenate(lanes, axis=1))
        lines = halves(jnp.concatenate(rows, axis=0))
        lines = [dot_split(lines, (table_ref[p], table_ref[2 + p])) for p in range(2)]
        planes = jnp.concatenate(
            [jnp.concatenate([lines[p][64 * j : 64 * j + 64] for p in range(2)], axis=0) for j in range(3)],
            axis=1,
        )
        high, low = halves(planes)
        planes = dot(table_ref[8], jnp.concatenate([high, high], axis=0)) + dot(table_ref[8, :, :128], low)
        images_re = []
        images_im = []
        for a in range(3):
            total_re = None
            for b in range(3):
                m = SYMMETRIC[a][b]
                kernel_re, kernel_im = [
                    jnp.concatenate(
                        [green_ref[pl.ds(8 * NZ * m + 4 * p + 2 * h + ky, NZ, stride=8), :] for h in range(2)],
                        axis=1,
                    )
                    for p in range(2)
                ]
                source_re = planes[:NZ, b * NX : (b + 1) * NX]
                source_im = planes[NZ:, b * NX : (b + 1) * NX]
                term_re = kernel_re * source_re - kernel_im * source_im
                term_im = kernel_re * source_im + kernel_im * source_re
                total_re = term_re if b == 0 else total_re + term_re
                total_im = term_im if b == 0 else total_im + term_im
            images_re.append(total_re)
            images_im.append(total_im)
        images = jnp.concatenate(
            [jnp.concatenate(images_re, axis=1), jnp.concatenate(images_im, axis=1)], axis=0
        )
        planes = dot_split((table_ref[9, :128], table_ref[9, 128:]), halves(images))
        lines = None
        for p in range(2):
            part = jnp.concatenate(
                [planes[64 * p : 64 * p + 64, j * NX : (j + 1) * NX] for j in range(3)], axis=0
            )
            part = dot_split(halves(part), (table_ref[4 + p], table_ref[6 + p]))
            lines = part if p == 0 else lines + part
        for j in range(3):
            for p in range(2):
                for zp in range(2):
                    first = 64 * j + BLOCKS * zp
                    out_ref[pl.ds(base + 6 * zp + 2 * j + p, BLOCKS, stride=48), :] = lines[
                        first : first + BLOCKS, p * LX : (p + 1) * LX
                    ]


def y_back_kernel(received_ref, places_ref, table_ref, out_ref):
    slots = 2 * DEVICES
    column = slot_places(places_ref[...])
    y = grid_index((slots, NY // 2), 1)
    hot = jnp.concatenate([(y == column).astype(BF16), (y + NY // 2 == column).astype(BF16)], axis=0)
    lefts = []
    for part in range(2):
        table = dot(hot, table_ref[256 + 64 * part : 320 + 64 * part, :]).astype(BF16)
        cos = table[:, :128]
        sin = table[:, 128:]
        c0, c1, s0, s1 = cos[:slots], cos[slots:], sin[:slots], sin[slots:]
        lefts.append(
            jnp.concatenate(
                [
                    jnp.concatenate([c0, c1, -s0, -s1], axis=1),
                    jnp.concatenate([s0, s1, c0, c1], axis=1),
                ],
                axis=0,
            )
        )
    rights = []
    for j in range(3):
        pieces = []
        for p in range(2):
            for zp in range(2):
                pieces.append(received_ref[pl.ds(6 * zp + 2 * j + p, NY, stride=12), :])
        rights.append(jnp.concatenate(pieces, axis=0))
    right = halves(jnp.concatenate(rights, axis=1))
    result = dot_split(lefts, right)
    for p in range(2):
        for t in range(2):
            for j in range(3):
                first = p * slots + t * DEVICES
                out_ref[pl.ds(6 * t + 2 * j + p, DEVICES, stride=12), :] = result[
                    first : first + DEVICES, j * 128 : (j + 1) * 128
                ]


def finish_kernel(received_ref, site_ref, dipoles_ref, alpha_ref, out_ref):
    target, _ = row_targets(site_ref)
    n = target.shape[1]
    target = to_column(target)
    hot = (grid_index((n, n), 1) == target).astype(BF16)
    live = target >= 0
    alpha_re = alpha_ref[:, :LX]
    alpha_im = alpha_ref[:, LX:]
    for c in range(6):
        v, j = divmod(c, 3)
        lanes = []
        for p in range(2):
            lanes.append(
                jnp.concatenate(
                    [
                        received_ref[pl.ds(12 * v + 6 * t + 2 * j + p, BLOCKS, stride=24), :]
                        for t in range(2)
                    ],
                    axis=0,
                )
            )
        rows = pick_rows(hot, jnp.concatenate(lanes, axis=1))
        dip_re = dipoles_ref[c, :, :LX]
        dip_im = dipoles_ref[c, :, LX:]
        out_ref[c, :, :LX] = jnp.where(live, alpha_re * dip_re - alpha_im * dip_im - rows[:, :LX], 0.0)
        out_ref[c, :, LX:] = jnp.where(live, alpha_re * dip_im + alpha_im * dip_re - rows[:, LX:], 0.0)


def call(kernel, shape, *operands, megabytes, flops=0, **more):
    whole = pl.BlockSpec(memory_space=pltpu.VMEM)
    options = dict(
        out_shape=shape and jax.ShapeDtypeStruct(shape, F32),
        in_specs=[whole] * len(operands),
        out_specs=whole,
        compiler_params=pltpu.CompilerParams(vmem_limit_bytes=megabytes * 1024 * 1024),
        cost_estimate=pl.CostEstimate(flops=2000000000, bytes_accessed=20000000, transcendentals=0),
        interpret=INTERPRET,
    )
    return pl.pallas_call(kernel, **{**options, **more})(*operands)


def exchange(rows):
    packed = rows.reshape(DEVICES, 1, rows.shape[0] // DEVICES * rows.shape[1])
    moved = lax.all_to_all(packed, "slab", split_axis=0, concat_axis=0, tiled=True)
    return moved.reshape(rows.shape)


def body(dipoles, inv_alpha, row_site, green):
    y_table, table = tables()
    packed = call(pack_kernel, (13 * DEVICES, LX), row_site, dipoles, megabytes=4)
    first = exchange(packed)
    planes, places = call(
        y_forward_kernel,
        None,
        first,
        y_table,
        megabytes=8,
        out_shape=(
            jax.ShapeDtypeStruct((24 * DEVICES, LX), F32),
            jax.ShapeDtypeStruct((DEVICES, LX), F32),
        ),
        out_specs=(pl.BlockSpec(memory_space=pltpu.VMEM), pl.BlockSpec(memory_space=pltpu.VMEM)),
    )
    pencils = exchange(planes)
    green_rows = green.reshape(6, NZ, 2, 4, LX).transpose(0, 1, 3, 2, 4).reshape(48 * NZ, LX)
    images = call(middle_kernel, (24 * DEVICES, LX), pencils, green_rows, table, megabytes=16)
    planes = exchange(images)
    rows = call(y_back_kernel, (12 * DEVICES, LX), planes, places, y_table, megabytes=8)
    returned = exchange(rows)
    return call(finish_kernel, dipoles.shape, returned, row_site, dipoles, inv_alpha, megabytes=4)


def solution(mesh):
    return jax.shard_map(
        body,
        mesh=mesh,
        in_specs=(
            P("rep", "slab", None),
            P("slab", None),
            P(None, "slab"),
            P(None, None, "slab", None),
        ),
        out_specs=P("rep", "slab", None),
        check_vma=False,
    )
```

```python
import math

import jax
import jax.numpy as jnp
import numpy as np
from jax import lax
from jax.experimental import pallas as pl
from jax.experimental.pallas import tpu as pltpu
from jax.sharding import PartitionSpec as P

NX = 256
NY = 128
NZ = 128
LX = 128
CHIPS = 32
SLOTS = 128
INTERPRET = False

F32 = jnp.float32
BF16 = jnp.bfloat16


def split_table(table):
    high = np.asarray(table, np.float32).astype(BF16)
    low = (table - high.astype(np.float64)).astype(np.float32).astype(BF16)
    return high, low


def phases(rows, columns, length, sign):
    angles = 2.0 * math.pi * (np.outer(rows, columns) % length) / length
    return np.cos(angles), sign * np.sin(angles)


def y_tables(core):
    y = np.arange(NY // 2)
    ky = np.arange(NY) ^ (2 * core)
    cos, sin = phases(ky, y, NY, -1.0)
    y_high, y_low = split_table(np.concatenate([cos, sin]))
    y_forward = np.concatenate([y_high, y_low])
    cos, sin = phases(y, ky, NY, 1.0)
    y_high, y_low = split_table(np.concatenate([cos, sin], axis=1) / NY)
    y_back = np.concatenate([y_high, y_low], axis=1)
    y_rows = np.zeros((384, 256), BF16)
    y_rows[:256, :64] = y_forward[:256]
    y_rows[:256, 64:128] = y_forward[256:]
    y_rows[256:320] = y_back[:, :256]
    y_rows[320:384] = y_back[:, 256:]
    return y_rows


def xz_table():
    z = np.concatenate([np.arange(0, NZ // 2, 2), np.arange(1, NZ // 2, 2)])
    kz = np.arange(NZ)
    x = np.arange(LX)
    kx = np.arange(NX)
    cos, sin = phases(x, kx, NX, -1.0)
    x_forward = split_table(np.block([[cos, sin], [-sin, cos]]))
    cos, sin = phases(kx, x, NX, 1.0)
    x_back = split_table(np.block([[cos, sin], [-sin, cos]]) / NX)
    cos, sin = phases(kz, z, NZ, -1.0)
    z_forward = split_table(np.block([[cos, -sin], [sin, cos]]))
    cos, sin = phases(z, kz, NZ, 1.0)
    z_back = split_table(np.block([[cos, -sin], [sin, cos]]) / NZ)
    pieces = []
    for part in x_forward:
        pieces += [part[:, :NX], part[:, NX:]]
    for part in x_back:
        pieces += [part[:NX], part[NX:]]
    pieces.append(np.concatenate(z_forward, axis=1))
    pieces.append(np.concatenate(z_back, axis=0))
    return np.stack(pieces)


def halves(values):
    high = values.astype(BF16)
    return high, (values - high.astype(F32)).astype(BF16)


def thirds(values):
    high = values.astype(BF16)
    rest = values - high.astype(F32)
    middle = rest.astype(BF16)
    return high, middle, (rest - middle.astype(F32)).astype(BF16)


def dot(left, right):
    return jnp.dot(left, right, preferred_element_type=F32)


def dot_split(left, right):
    return dot(left[0], right[0]) + (dot(left[0], right[1]) + dot(left[1], right[0]))


def pick_rows(hot, values):
    high, middle, low = thirds(values)
    return dot(hot, high) + dot(hot, middle) + dot(hot, low)


def grid_index(shape, axis):
    return lax.broadcasted_iota(jnp.int32, shape, axis)


def to_column(row):
    n = row.shape[1]
    diagonal = grid_index((n, n), 0) == grid_index((n, n), 1)
    return jnp.sum(jnp.where(diagonal, row, 0), axis=1, keepdims=True)


def row_targets(site_ref):
    cell_y = site_ref[0:1, :]
    cell_z = site_ref[1:2, :]
    block = jnp.where(cell_y >= 0, cell_z // 2, -1)
    n = block.shape[1]
    earlier = grid_index((n, n), 0) < grid_index((n, n), 1)
    same = (to_column(block) == block) & earlier
    rank = jnp.sum(same.astype(jnp.int32), axis=0, keepdims=True)
    target = jnp.where(cell_y >= 0, rank * CHIPS + block, -1)
    return target, (cell_z % 2) * (NY // 2) + cell_y


def my_core():
    return lax.axis_index("slab") % 2


def pack_rows(site_ref, rows, side, out_ref):
    target, place = row_targets(site_ref)
    n = target.shape[1]
    chosen = grid_index((n, n), 0) == target
    hot = chosen.astype(BF16)
    for j in range(3):
        picked = pick_rows(hot, rows(j))
        for t in range(2):
            for p in range(2):
                out_ref[pl.ds(6 * (2 * side + t) + 2 * j + p, CHIPS, stride=25), :] = picked[
                    t * CHIPS : (t + 1) * CHIPS, p * LX : (p + 1) * LX
                ]
    places = jnp.sum(jnp.where(chosen, place + 1, 0), axis=1, keepdims=True) - 1
    places = places.astype(F32)
    lanes = grid_index((CHIPS, LX), 1)
    return jnp.where(lanes % 2 == 0, places[:CHIPS], places[CHIPS:])


def pack_own_kernel(site_ref, dipoles_ref, out_ref):
    core = my_core()
    row = pack_rows(site_ref, lambda j: dipoles_ref[3 * core + j], 0, out_ref)
    out_ref[pl.ds(24, CHIPS, stride=25), :] = row


def pack_other_kernel(own_ref, site_ref, dipoles_ref, out_ref):
    core = my_core()
    out_ref[...] = own_ref[...]
    row = pack_rows(site_ref, lambda j: dipoles_ref[3 * core + j], 1, out_ref)
    lanes = grid_index((CHIPS, LX), 1)
    own_row = own_ref[pl.ds(24, CHIPS, stride=25), :]
    out_ref[pl.ds(24, CHIPS, stride=25), :] = jnp.where(lanes < 2, own_row, row)


def slot_places(rows):
    return jnp.concatenate([rows[:, t : t + 1] for t in range(4)], axis=0).astype(jnp.int32)


def y_forward_kernel(received_ref, table_ref, out_ref, places_ref):
    slots = SLOTS
    core = my_core()
    places = received_ref[pl.ds(24, CHIPS, stride=25), :]
    places_ref[...] = places
    column = slot_places(places)
    diagonal = grid_index((slots, slots), 0) == grid_index((slots, slots), 1)
    row = jnp.sum(jnp.where(diagonal, column, 0), axis=0, keepdims=True)
    y = grid_index((NY // 2, slots), 0)
    hot = jnp.concatenate([(y == row).astype(BF16), (y + NY // 2 == row).astype(BF16)], axis=1)
    none = jnp.zeros_like(hot)
    lefts = []
    for part in range(2):
        chooser = jnp.concatenate([none, hot] if part else [hot, none], axis=0)
        table = dot(table_ref[core, :256, :128], chooser).astype(BF16)
        cos = table[:128]
        sin = table[128:]
        rows = []
        for zp in range(2):
            c = cos[:, zp * slots : (zp + 1) * slots]
            s = sin[:, zp * slots : (zp + 1) * slots]
            rows.append(jnp.concatenate([c, -s], axis=1))
            rows.append(jnp.concatenate([s, c], axis=1))
        lefts.append(jnp.concatenate(rows, axis=0))
    rights = []
    for j in range(3):
        pieces = []
        for p in range(2):
            for t in range(4):
                pieces.append(received_ref[pl.ds(6 * t + 2 * j + p, CHIPS, stride=25), :])
        rights.append(jnp.concatenate(pieces, axis=0))
    right = halves(jnp.concatenate(rights, axis=1))
    result = dot_split(lefts, right)
    for zp in range(2):
        for p in range(2):
            for j in range(3):
                out_ref[pl.ds(6 * zp + 2 * j + p, NY, stride=12), :] = result[
                    zp * 256 + p * 128 : zp * 256 + p * 128 + 128, j * 128 : (j + 1) * 128
                ]


SYMMETRIC = ((0, 1, 2), (1, 3, 4), (2, 4, 5))


def middle_kernel(received_ref, own_green_ref, other_green_ref, table_ref, out_ref):
    for g in range(4):
        ky = g % 2
        green_ref = own_green_ref if g < 2 else other_green_ref
        base = 12 * g
        rows = []
        for j in range(3):
            lanes = []
            for p in range(2):
                lanes.append(
                    jnp.concatenate(
                        [
                            received_ref[pl.ds(base + 6 * zp + 2 * j + p, CHIPS, stride=48), :]
                            for zp in range(2)
                        ],
                        axis=0,
                    )
                )
            rows.append(jnp.concatenate(lanes, axis=1))
        lines = halves(jnp.concatenate(rows, axis=0))
        lines = [dot_split(lines, (table_ref[p], table_ref[2 + p])) for p in range(2)]
        planes = jnp.concatenate(
            [jnp.concatenate([lines[p][64 * j : 64 * j + 64] for p in range(2)], axis=0) for j in range(3)],
            axis=1,
        )
        high, low = halves(planes)
        planes = dot(table_ref[8], jnp.concatenate([high, high], axis=0)) + dot(table_ref[8, :, :128], low)
        images_re = []
        images_im = []
        for a in range(3):
            total_re = None
            for b in range(3):
                m = SYMMETRIC[a][b]
                kernel_re, kernel_im = [
                    jnp.concatenate(
                        [green_ref[pl.ds(8 * NZ * m + 4 * p + 2 * h + ky, NZ, stride=8), :] for h in range(2)],
                        axis=1,
                    )
                    for p in range(2)
                ]
                source_re = planes[:NZ, b * NX : (b + 1) * NX]
                source_im = planes[NZ:, b * NX : (b + 1) * NX]
                term_re = kernel_re * source_re - kernel_im * source_im
                term_im = kernel_re * source_im + kernel_im * source_re
                total_re = term_re if b == 0 else total_re + term_re
                total_im = term_im if b == 0 else total_im + term_im
            images_re.append(total_re)
            images_im.append(total_im)
        images = jnp.concatenate(
            [jnp.concatenate(images_re, axis=1), jnp.concatenate(images_im, axis=1)], axis=0
        )
        planes = dot_split((table_ref[9, :128], table_ref[9, 128:]), halves(images))
        lines = None
        for p in range(2):
            part = jnp.concatenate(
                [planes[64 * p : 64 * p + 64, j * NX : (j + 1) * NX] for j in range(3)], axis=0
            )
            part = dot_split(halves(part), (table_ref[4 + p], table_ref[6 + p]))
            lines = part if p == 0 else lines + part
        for j in range(3):
            for p in range(2):
                for zp in range(2):
                    first = 64 * j + CHIPS * zp
                    out_ref[pl.ds(base + 6 * zp + 2 * j + p, CHIPS, stride=48), :] = lines[
                        first : first + CHIPS, p * LX : (p + 1) * LX
                    ]


def y_back_kernel(received_ref, places_ref, table_ref, out_ref):
    slots = SLOTS
    core = my_core()
    column = slot_places(places_ref[...])
    y = grid_index((slots, NY // 2), 1)
    hot = jnp.concatenate([(y == column).astype(BF16), (y + NY // 2 == column).astype(BF16)], axis=0)
    lefts = []
    for part in range(2):
        table = dot(hot, table_ref[core, 256 + 64 * part : 320 + 64 * part, :]).astype(BF16)
        cos = table[:, :128]
        sin = table[:, 128:]
        c0, c1, s0, s1 = cos[:slots], cos[slots:], sin[:slots], sin[slots:]
        lefts.append(
            jnp.concatenate(
                [
                    jnp.concatenate([c0, c1, -s0, -s1], axis=1),
                    jnp.concatenate([s0, s1, c0, c1], axis=1),
                ],
                axis=0,
            )
        )
    rights = []
    for j in range(3):
        pieces = []
        for p in range(2):
            for zp in range(2):
                pieces.append(received_ref[pl.ds(6 * zp + 2 * j + p, NY, stride=12), :])
        rights.append(jnp.concatenate(pieces, axis=0))
    right = halves(jnp.concatenate(rights, axis=1))
    result = dot_split(lefts, right)
    for p in range(2):
        for t in range(4):
            for j in range(3):
                first = p * slots + t * CHIPS
                out_ref[pl.ds(6 * t + 2 * j + p, CHIPS, stride=24), :] = result[
                    first : first + CHIPS, j * 128 : (j + 1) * 128
                ]


def finish_rows(received_ref, side, site_ref, dipoles_ref, alpha_ref, out_ref):
    target, _ = row_targets(site_ref)
    n = target.shape[1]
    target = to_column(target)
    hot = (grid_index((n, n), 1) == target).astype(BF16)
    live = target >= 0
    alpha_re = alpha_ref[:, :LX]
    alpha_im = alpha_ref[:, LX:]
    core = my_core()
    for j in range(3):
        lanes = []
        for p in range(2):
            lanes.append(
                jnp.concatenate(
                    [
                        received_ref[pl.ds(6 * (2 * side + t) + 2 * j + p, CHIPS, stride=24), :]
                        for t in range(2)
                    ],
                    axis=0,
                )
            )
        rows = pick_rows(hot, jnp.concatenate(lanes, axis=1))
        c = 3 * (core if side == 0 else 1 - core) + j
        dip_re = dipoles_ref[c, :, :LX]
        dip_im = dipoles_ref[c, :, LX:]
        out_ref[j, :, :LX] = jnp.where(live, alpha_re * dip_re - alpha_im * dip_im - rows[:, :LX], 0.0)
        out_ref[j, :, LX:] = jnp.where(live, alpha_re * dip_im + alpha_im * dip_re - rows[:, LX:], 0.0)


def finish_own_kernel(received_ref, site_ref, dipoles_ref, alpha_ref, out_hbm, rows_ref, done):
    finish_rows(received_ref, 0, site_ref, dipoles_ref, alpha_ref, rows_ref)
    copy = pltpu.make_async_copy(rows_ref, out_hbm.at[pl.ds(3 * my_core(), 3)], done)
    copy.start()
    copy.wait()


def finish_other_kernel(received_ref, site_ref, dipoles_ref, alpha_ref, own_hbm, out_hbm, rows_ref, done):
    finish_rows(received_ref, 1, site_ref, dipoles_ref, alpha_ref, rows_ref)
    copy = pltpu.make_async_copy(rows_ref, out_hbm.at[pl.ds(3 - 3 * my_core(), 3)], done)
    copy.start()
    copy.wait()


def call(kernel, shape, *operands, megabytes, mflops=200, **more):
    whole = pl.BlockSpec(memory_space=pltpu.VMEM)
    options = dict(
        out_shape=shape and jax.ShapeDtypeStruct(shape, F32),
        in_specs=[whole] * len(operands),
        out_specs=whole,
        compiler_params=pltpu.CompilerParams(vmem_limit_bytes=megabytes * 1024 * 1024),
        cost_estimate=pl.CostEstimate(
            flops=mflops * 1000000, bytes_accessed=2000000, transcendentals=0
        ),
        interpret=INTERPRET,
    )
    return pl.pallas_call(kernel, **{**options, **more})(*operands)


def exchange(rows):
    packed = rows.reshape(CHIPS, 1, rows.shape[0] // CHIPS * rows.shape[1])
    groups = [[2 * chip + core for chip in range(CHIPS)] for core in range(2)]
    moved = lax.all_to_all(
        packed, "slab", split_axis=0, concat_axis=0, tiled=True, axis_index_groups=groups
    )
    return moved.reshape(rows.shape)


def swap(rows):
    return lax.ppermute(rows, "slab", [(d, d ^ 1) for d in range(2 * CHIPS)])


def body(dipoles, inv_alpha, row_site, green):
    y_table = np.stack([y_tables(core) for core in range(2)])
    table = xz_table()
    other_dipoles = swap(dipoles)
    other_site = swap(row_site)
    green_rows = green.reshape(6, NZ, 2, 4, LX).transpose(0, 1, 3, 2, 4).reshape(48 * NZ, LX)
    whole = pl.BlockSpec(memory_space=pltpu.VMEM)
    hbm = pl.BlockSpec(memory_space=pltpu.HBM)
    own_packed = call(pack_own_kernel, (25 * CHIPS, LX), row_site, dipoles, megabytes=4, mflops=2000)
    packed = call(
        pack_other_kernel, (25 * CHIPS, LX), own_packed, other_site, other_dipoles, megabytes=4, mflops=2000
    )
    first = exchange(packed)
    planes, places = call(
        y_forward_kernel,
        None,
        first,
        y_table,
        megabytes=8,
        mflops=1000,
        out_shape=(
            jax.ShapeDtypeStruct((48 * CHIPS, LX), F32),
            jax.ShapeDtypeStruct((CHIPS, LX), F32),
        ),
        out_specs=(pl.BlockSpec(memory_space=pltpu.VMEM), pl.BlockSpec(memory_space=pltpu.VMEM)),
    )
    planes, green_rows = lax.optimization_barrier((planes, green_rows))
    other_green = swap(green_rows)
    pencils = exchange(planes)
    images = call(
        middle_kernel, (48 * CHIPS, LX), pencils, green_rows, other_green, table, megabytes=16, mflops=2000
    )
    planes = exchange(images)
    rows = call(y_back_kernel, (24 * CHIPS, LX), planes, places, y_table, megabytes=8)
    returned = exchange(rows)
    other_returned = swap(returned)
    last = dict(
        megabytes=4,
        out_specs=hbm,
        scratch_shapes=[pltpu.VMEM((3,) + dipoles.shape[1:], F32), pltpu.SemaphoreType.DMA],
    )
    own = call(finish_own_kernel, dipoles.shape, returned, row_site, dipoles, inv_alpha, **last)
    return call(
        finish_other_kernel,
        dipoles.shape,
        other_returned,
        row_site,
        dipoles,
        inv_alpha,
        own,
        in_specs=[whole] * 4 + [hbm],
        input_output_aliases={4: 0},
        **last,
    )


def solution(mesh):
    return jax.shard_map(
        body,
        mesh=mesh,
        in_specs=(
            P("rep", "slab", None),
            P("slab", None),
            P(None, "slab"),
            P(None, None, "slab", None),
        ),
        out_specs=P("rep", "slab", None),
        check_vma=False,
    )
```
